128 devices in a mesh: shard: 32 (over z, y, x_lo), model: 4 (over x_hi, core).
Axes of the slice: x: 4 (x_hi: 2, x_lo: 2; x = x_hi * 2 + x_lo), y: 4, z: 4, core: 2. Of those that a mesh axis runs over, the one named last changes fastest.
Arguments:
- w_query: bfloat16 [12288, 12288], P('shard', 'model'), may hold values from -0.109375 to 0.109375
- low_query: bfloat16 [12288, 16], P('shard'), may hold values from -0.0546875 to 0.0546875
- high_query: bfloat16 [16, 12288], P(None, 'model'), may hold values from -1.5 to 1.5
- w_key: bfloat16 [12288, 12288], P('shard', 'model'), may hold values from -0.109375 to 0.109375
- low_key: bfloat16 [12288, 16], P('shard'), may hold values from -0.0546875 to 0.0546875
- high_key: bfloat16 [16, 12288], P(None, 'model'), may hold values from -1.5 to 1.5
- w_value: bfloat16 [12288, 12288], P('shard', 'model'), may hold values from -0.109375 to 0.109375
- low_value: bfloat16 [12288, 16], P('shard'), may hold values from -0.0546875 to 0.0546875
- high_value: bfloat16 [16, 12288], P(None, 'model'), may hold values from -1.5 to 1.5
- norm_gain: float32 [12288], P('shard'), may hold values from 0.25 to 1.75
Outputs:
- final_query: bfloat16 [12288, 12288], P(None, ('model', 'shard'))
- final_key: bfloat16 [12288, 12288], P(None, ('model', 'shard'))
- final_value: bfloat16 [12288, 12288], P(None, ('model', 'shard'))
- scale_query: float32 [12288], P(('model', 'shard'))
- scale_key: float32 [12288], P(('model', 'shard'))
- scale_value: float32 [12288], P(('model', 'shard'))
The draws below stay inside these ranges and needn't reach their ends.
All inputs are finite; a program needn't handle non-finite values. Where the reference program divides by a largest or mean magnitude, that divisor is 1e-20 or more.
Results may differ from the reference program's by a relative error of at most 0.001.
Values may be sent and summed in bfloat16 or wider, within the bound.
A program may use at most 128 MiB of HBM per device.

```python
import jax
import jax.numpy as jnp

D_MODEL = 12288
Q_DIM = 12288
KV_DIM = 12288
RANK = 16


def with_spikes(values, key, source, target, blocks, factor):
    def block_of(dim):
        return (jnp.arange(values.shape[dim]) // (values.shape[dim] // blocks)).reshape((-1,) + (1,) * (values.ndim - 1 - dim))

    near = jax.random.permutation(key, blocks)[block_of(target)]
    second = (block_of(target) + blocks // 2) % blocks
    return jnp.where((block_of(source) == near) | (block_of(source) == second), factor * values, values)


def shard_levels(stream_key, extent, split, low, largest):
    gain, own = 1.0, jax.random.fold_in(stream_key, 6)
    for position, blocks in split:
        steps = jnp.exp(jax.random.uniform(jax.random.fold_in(own, position), (blocks,), jnp.float32, low / len(split), largest / len(split)))
        gain = gain * jnp.repeat(steps, extent[position] // blocks).reshape([-1 if axis == position else 1 for axis in range(len(extent))])
    return gain


def normal_values(stream_key, extent, width, reach, shards=(), dtype=jnp.bfloat16):
    entries = jax.random.normal(stream_key, extent, jnp.float32) * width
    if len(shards) > 0:
        entries = shard_levels(stream_key, extent, shards, -0.22, 0.18) * entries
    return jnp.clip(entries, min=-reach, max=reach).astype(dtype)


def heavy_noise(rng, extent, width, reach, cuts, heavy, kind=jnp.bfloat16):
    values = width * jax.random.normal(rng, extent, jnp.float32)
    if cuts:
        values = values * shard_levels(rng, extent, cuts, -0.22, 0.18)
    return jnp.clip(with_spikes(values, jax.random.fold_in(rng, 3), *heavy), -reach, reach).astype(kind)


def setup_inputs(seed: int = 0) -> dict:
    streams_of = jax.random.split(jax.random.key(seed), 11)
    w_query = heavy_noise(streams_of[0], (D_MODEL, Q_DIM), D_MODEL ** -0.5, 0.109375, ((0, 32), (1, 4)), (0, 1, 32, 2.75))
    low_query = normal_values(streams_of[1], (D_MODEL, RANK), D_MODEL ** -0.5, 0.0546875, ((0, 32),))
    high_query = normal_values(streams_of[2], (RANK, Q_DIM), RANK ** -0.5, 1.5, ((1, 4),))
    w_key = heavy_noise(streams_of[3], (D_MODEL, KV_DIM), D_MODEL ** -0.5, 0.109375, ((0, 32), (1, 4)), (0, 1, 32, 2.75))
    low_key = normal_values(streams_of[4], (D_MODEL, RANK), D_MODEL ** -0.5, 0.0546875, ((0, 32),))
    high_key = normal_values(streams_of[5], (RANK, KV_DIM), RANK ** -0.5, 1.5, ((1, 4),))
    w_value = heavy_noise(streams_of[6], (D_MODEL, KV_DIM), D_MODEL ** -0.5, 0.109375, ((0, 32), (1, 4)), (0, 1, 32, 2.75))
    low_value = normal_values(streams_of[7], (D_MODEL, RANK), D_MODEL ** -0.5, 0.0546875, ((0, 32),))
    high_value = normal_values(streams_of[8], (RANK, KV_DIM), RANK ** -0.5, 1.5, ((1, 4),))
    norm_gain = jnp.clip(1.0 + 0.15 * jax.random.normal(streams_of[9], (D_MODEL,), jnp.float32), 0.25, 1.75)
    return dict(w_query=w_query, low_query=low_query, high_query=high_query, w_key=w_key, low_key=low_key, high_key=high_key, w_value=w_value, low_value=low_value, high_value=high_value, norm_gain=norm_gain)


mix_rate = 1.0


def reference(w_query, low_query, high_query, w_key, low_key, high_key, w_value, low_value, high_value, norm_gain):
    result_query = w_query.astype(jnp.float32) + mix_rate * jnp.dot(low_query, high_query, preferred_element_type=jnp.float32)
    result_key = w_key.astype(jnp.float32) + mix_rate * jnp.dot(low_key, high_key, preferred_element_type=jnp.float32)
    result_value = w_value.astype(jnp.float32) + mix_rate * jnp.dot(low_value, high_value, preferred_element_type=jnp.float32)
    result_gained_query = result_query * norm_gain[:, None]
    result_gained_key = result_key * norm_gain[:, None]
    result_gained_value = result_value * norm_gain[:, None]
    scale_query = jnp.max(jnp.abs(result_gained_query), axis=0)
    final_query = (result_gained_query / scale_query).astype(jnp.bfloat16)
    scale_key = jnp.max(jnp.abs(result_gained_key), axis=0)
    final_key = (result_gained_key / scale_key).astype(jnp.bfloat16)
    scale_value = jnp.max(jnp.abs(result_gained_value), axis=0)
    final_value = (result_gained_value / scale_value).astype(jnp.bfloat16)
    return final_query, final_key, final_value, scale_query, scale_key, scale_value
```

```python
import functools

import jax
import jax.numpy as jnp
from jax import lax
from jax.experimental import pallas as pl
from jax.experimental.pallas import tpu as pltpu
from jax.sharding import PartitionSpec as P

MESH = pl.DeviceIdType.MESH

NZ, NY, NX = 4, 4, 2
N = NZ * NY * NX
PARTS = 2


def hops(offset):
    dz, dy, dx = offset
    return min(dz, NZ - dz) + min(dy, NY - dy) + dx


OFFSETS = sorted(
    [(dz, dy, dx) for dz in range(NZ) for dy in range(NY) for dx in range(NX)][1:],
    key=lambda o: -hops(o),
)
PLANE = [(dz, dy) for dz in range(NZ) for dy in range(NY)][1:]


def exchange(*refs):
    (wq, wk, wv, lq, lk, lv, hq, hk, hv, gain_ref) = refs[:10]
    (out, scale_out) = refs[10:12]
    (wbuf, wt, land, gbuf, low_all, gain_all, ht, hrow) = refs[12:20]
    (load_sem, send_sem, recv_sem, low_send, low_recv, gain_send, gain_recv, relay_send, relay_gain) = refs[20:]
    rows = wq.shape[0]
    cols = land.shape[1]
    step = cols // PARTS
    rank = lq.shape[0]
    me = lax.axis_index("shard")
    mine = lax.axis_index("model")
    core = lax.rem(mine, 2)
    z, y, x = me // (NY * NX), lax.rem(me // NX, NY), lax.rem(me, NX)

    def there(offset):
        dz, dy, dx = offset
        return lax.rem(z + dz, NZ) * (NY * NX) + lax.rem(y + dy, NY) * NX + lax.rem(x + dx, NX)

    loads = []
    for m, w in enumerate((wq, wk, wv)):
        load = pltpu.make_async_copy(w, wbuf.at[m], load_sem.at[m])
        load.start()
        loads.append(load)

    other_core = {"model": mine + 1 - 2 * core}
    across = {"shard": me + 1 - 2 * x, "model": lax.rem(mine + 2, 4)}
    barrier = pltpu.get_barrier_semaphore()
    for o in OFFSETS:
        pl.semaphore_signal(barrier, inc=1, device_id={"shard": there(o)}, device_id_type=MESH)
    pl.semaphore_signal(barrier, inc=1, device_id=other_core, device_id_type=MESH)
    pl.semaphore_signal(barrier, inc=1, device_id=across, device_id_type=MESH)

    at_me = pl.ds(pl.multiple_of(me * rows, rows), rows)
    group = 4 * cols
    for m, (l, h) in enumerate(((lq, hq), (lk, hk), (lv, hv))):
        low_all[m, :, at_me] = l[...]
        part = h[:, pl.ds(pl.multiple_of((me // 4) * group, group), group)]
        hrow[...] = part.astype(jnp.float32).T
        ht[m] = hrow[pl.ds(pl.multiple_of(lax.rem(me, 4) * cols, 8), cols), :].astype(jnp.bfloat16)
    gain_all[:, at_me] = gain_ref[...].reshape(1, rows)

    for m in range(3):
        loads[m].wait()

        def turn(g, _):
            at = pl.ds(pl.multiple_of(g * group, group), group)
            wt[m, at, :] = wbuf[m, :, at].T
            return 0

        lax.fori_loop(0, wbuf.shape[2] // group, turn, 0)
        land[m, :, at_me] = wt[m, pl.ds(pl.multiple_of(me * cols, 16), cols), :]

    pl.semaphore_wait(barrier, N + 1)

    def low_copy(owner, send, recv, target):
        at = pl.ds(pl.multiple_of(owner * rows, rows), rows)
        return pltpu.make_async_remote_copy(
            src_ref=low_all.at[:, :, at], dst_ref=low_all.at[:, :, at],
            send_sem=send, recv_sem=recv, device_id=target, device_id_type=MESH,
        )

    def gain_copy(owner, send, recv, target):
        at = pl.ds(pl.multiple_of(owner * rows, rows), rows)
        return pltpu.make_async_remote_copy(
            src_ref=gain_all.at[:, at], dst_ref=gain_all.at[:, at],
            send_sem=send, recv_sem=recv, device_id=target, device_id_type=MESH,
        )

    for i, (dz, dy) in enumerate(PLANE):
        @pl.when(core == (dz + dy) % 2)
        def _():
            target = {"shard": there((dz, dy, 0))}
            low_copy(me, low_send.at[i], low_recv.at[me], target).start()
            gain_copy(me, gain_send.at[i], gain_recv.at[me], target).start()
    low_copy(me, relay_send.at[0, 0], low_recv.at[me], across).start()
    gain_copy(me, relay_gain.at[0, 0], gain_recv.at[me], across).start()

    def block_copy(m, p, i, o):
        t = there(o)
        at = pl.ds(pl.multiple_of(me * rows, rows), rows)
        return pltpu.make_async_remote_copy(
            src_ref=wt.at[m, pl.ds(pl.multiple_of(t * cols + p * step, 16), step), :],
            dst_ref=land.at[m, pl.ds(pl.multiple_of(p * step, 16), step), at],
            send_sem=send_sem.at[m * PARTS + p, i],
            recv_sem=recv_sem.at[m * PARTS + p, me],
            device_id={"shard": t}, device_id_type=MESH,
        )

    def send_slot(slot, _):
        m, p = slot // PARTS, lax.rem(slot, PARTS)
        for i, o in enumerate(OFFSETS):
            block_copy(m, p, i, o).start()
        return 0

    lax.fori_loop(0, 3 * PARTS, send_slot, 0)

    for i, (dz, dy) in enumerate(PLANE):
        @pl.when(core == (dz + dy) % 2)
        def _():
            owner = there((NZ - dz, NY - dy, 0))
            low_copy(owner, low_send.at[i], low_recv.at[owner], other_core).wait_recv()
            gain_copy(owner, gain_send.at[i], gain_recv.at[owner], other_core).wait_recv()
            for k, target in ((1, other_core), (2, across)):
                low_copy(owner, relay_send.at[k, i + 1], low_recv.at[owner], target).start()
                gain_copy(owner, relay_gain.at[k, i + 1], gain_recv.at[owner], target).start()
    flip = 1 - 2 * x
    for i, (dz, dy) in enumerate(PLANE):
        @pl.when(core == (dz + dy) % 2)
        def _():
            owner = there((NZ - dz, NY - dy, 0)) + flip
            low_copy(owner, low_send.at[i], low_recv.at[owner], other_core).wait_recv()
            gain_copy(owner, gain_send.at[i], gain_recv.at[owner], other_core).wait_recv()
            low_copy(owner, relay_send.at[3, i + 1], low_recv.at[owner], other_core).start()
            gain_copy(owner, relay_gain.at[3, i + 1], gain_recv.at[owner], other_core).start()
    low_copy(me + flip, relay_send.at[0, 0], low_recv.at[me + flip], other_core).wait_recv()
    gain_copy(me + flip, relay_gain.at[0, 0], gain_recv.at[me + flip], other_core).wait_recv()
    for i, (dz, dy) in enumerate(PLANE):
        @pl.when(core != (dz + dy) % 2)
        def _():
            for owner in (there((NZ - dz, NY - dy, 0)), there((NZ - dz, NY - dy, 0)) + flip):
                low_copy(owner, low_send.at[i], low_recv.at[owner], other_core).wait_recv()
                gain_copy(owner, gain_send.at[i], gain_recv.at[owner], other_core).wait_recv()

    for m in range(3):
        for p in range(PARTS):
            lines = slice(p * step, (p + 1) * step)
            slot = m * PARTS + p

            def gained(source):
                at = pl.ds(pl.multiple_of(source * rows, rows), rows)
                update = jnp.dot(ht[m, lines, :], low_all[m, :, at], preferred_element_type=jnp.float32)
                r = (land[m, lines, at].astype(jnp.float32) + update) * gain_all[:, at]
                gbuf[lines, at] = r
                a = jnp.abs(r)
                return jnp.maximum(jnp.maximum(a[:, 0:128], a[:, 128:256]), a[:, 256:384])

            top = gained(me)

            def collect(i, top):
                source = lax.rem(me + 1 + i, N)
                at = pl.ds(pl.multiple_of(source * rows, rows), rows)
                pltpu.make_async_remote_copy(
                    src_ref=wt.at[m, pl.ds(0, step), :],
                    dst_ref=land.at[m, pl.ds(p * step, step), at],
                    send_sem=send_sem.at[slot, 0], recv_sem=recv_sem.at[slot, source],
                    device_id=other_core, device_id_type=MESH,
                ).wait_recv()
                return jnp.maximum(top, gained(source))

            top = lax.fori_loop(0, N - 1, collect, top)
            scale = jnp.max(top, axis=1, keepdims=True)
            scale_out[m, lines, :] = jnp.broadcast_to(scale, (step, 128))
            inverse = 1.0 / scale

            def finish(source, _):
                at = pl.ds(pl.multiple_of(source * rows, rows), rows)
                out[m, lines, at] = (gbuf[lines, at] * inverse).astype(out.dtype)
                return 0

            lax.fori_loop(0, N, finish, 0)

    def sent_slot(slot, _):
        m, p = slot // PARTS, lax.rem(slot, PARTS)
        for i, o in enumerate(OFFSETS):
            block_copy(m, p, i, o).wait_send()
        return 0

    lax.fori_loop(0, 3 * PARTS, sent_slot, 0)
    low_copy(me, relay_send.at[0, 0], low_recv.at[me], across).wait_send()
    gain_copy(me, relay_gain.at[0, 0], gain_recv.at[me], across).wait_send()
    for i, (dz, dy) in enumerate(PLANE):
        @pl.when(core == (dz + dy) % 2)
        def _():
            low_copy(me, low_send.at[i], low_recv.at[me], other_core).wait_send()
            gain_copy(me, gain_send.at[i], gain_recv.at[me], other_core).wait_send()
            for k in (1, 2, 3):
                low_copy(me, relay_send.at[k, i + 1], low_recv.at[me], other_core).wait_send()
                gain_copy(me, relay_gain.at[k, i + 1], gain_recv.at[me], other_core).wait_send()


def deliver(out, scale, fq, fk, fv, sq, sk, sv, row, sem):
    copies = []
    for m, f in enumerate((fq, fk, fv)):
        copy = pltpu.make_async_copy(out.at[m], f, sem.at[m])
        copy.start()
        copies.append(copy)
    for m, s in enumerate((sq, sk, sv)):
        s[...] = scale[m].T[0:1, :]
    for copy in copies:
        copy.wait()


def on_device(wq, lq, hq, wk, lk, hk, wv, lv, hv, gain):
    rows, width = wq.shape
    rank = lq.shape[1]
    cols = width // N
    total = rows * N
    f32, bf16 = jnp.float32, jnp.bfloat16
    vmem = pl.BlockSpec(memory_space=pltpu.VMEM)
    anywhere = pl.BlockSpec(memory_space=pl.ANY)
    dma = pltpu.SemaphoreType.DMA
    out, scale = pl.pallas_call(
        exchange,
        out_shape=(
            pltpu.VMEM((3, cols, total), bf16),
            pltpu.VMEM((3, cols, 128), f32),
        ),
        in_specs=[anywhere] * 3 + [vmem] * 7,
        out_specs=(vmem, vmem),
        scratch_shapes=[
            pltpu.VMEM((3, rows, width), bf16),
            pltpu.VMEM((3, width, rows), bf16),
            pltpu.VMEM((3, cols, total), bf16),
            pltpu.VMEM((cols, total), f32),
            pltpu.VMEM((3, rank, total), bf16),
            pltpu.VMEM((1, total), f32),
            pltpu.VMEM((3, cols, rank), bf16),
            pltpu.VMEM((4 * cols, rank), f32),
            dma((3,)),
            dma((3 * PARTS, N)),
            dma((3 * PARTS, N)),
            dma((16,)),
            dma((N,)),
            dma((16,)),
            dma((N,)),
            dma((4, 16)),
            dma((4, 16)),
        ],
        compiler_params=pltpu.CompilerParams(
            collective_id=0, has_side_effects=True, vmem_limit_bytes=52 * 2**20
        ),
    )(wq, wk, wv, lq.T, lk.T, lv.T, hq, hk, hv, gain)
    final = jax.ShapeDtypeStruct((cols, total), bf16)
    line = jax.ShapeDtypeStruct((1, cols), f32)
    fq, fk, fv, sq, sk, sv = pl.pallas_call(
        deliver,
        out_shape=(final, final, final, line, line, line),
        in_specs=[vmem, vmem],
        out_specs=(anywhere,) * 3 + (vmem,) * 3,
        scratch_shapes=[pltpu.VMEM((8, 128), f32), dma((3,))],
        compiler_params=pltpu.CompilerParams(vmem_limit_bytes=2 * 2**20),
    )(
        pltpu.with_memory_space_constraint(out, pltpu.VMEM),
        pltpu.with_memory_space_constraint(scale, pltpu.VMEM),
    )
    return fq.T, fk.T, fv.T, sq.reshape(cols), sk.reshape(cols), sv.reshape(cols)


def solution(mesh):
    weight, low, high = P("shard", "model"), P("shard", None), P(None, "model")
    final, scale = P(None, ("model", "shard")), P(("model", "shard"))
    return jax.shard_map(
        on_device,
        mesh=mesh,
        in_specs=(weight, low, high) * 3 + (P("shard"),),
        out_specs=(final,) * 3 + (scale,) * 3,
        check_vma=False,
    )
```

```python
import jax
import jax.numpy as jnp
from jax import lax
from jax.experimental import pallas as pl
from jax.experimental.pallas import tpu as pltpu
from jax.sharding import PartitionSpec as P

MESH = pl.DeviceIdType.MESH

NZ, NY, NX = 4, 4, 2
N = NZ * NY * NX
CUTS = (((0, 3), (3, 3)), ((0, 3), (3, 3)), ((0, 3), (3, 3)))
SLOTS = [(m, a, n) for m, cuts in enumerate(CUTS) for a, n in cuts]
CHUNKS = 8


def hops(offset):
    dz, dy, dx = offset
    return min(dz, NZ - dz) + min(dy, NY - dy) + dx


OFFSETS = sorted(
    [(dz, dy, dx) for dz in range(NZ) for dy in range(NY) for dx in range(NX)][1:],
    key=lambda o: -hops(o),
)
PLANE = [(dz, dy) for dz in range(NZ) for dy in range(NY)][1:]


def exchange(*refs):
    weights, lows, highs, gain_ref = refs[0:3], refs[3:6], refs[6:9], refs[9]
    out, scale_out = refs[10:12]
    (wbuf, wt, land, gbuf, low_all, gain_all, ht, hrow, hbuf, gbuf_in) = refs[12:22]
    (load_sem, small_sem, send_sem, recv_sem, low_send, low_recv, gain_send, gain_recv) = refs[22:]
    rows = wbuf.shape[1]
    cols = land.shape[1]
    unit = cols // 6
    group = 4 * cols
    groups = wbuf.shape[2] // group
    me = lax.axis_index("shard")
    mine = lax.axis_index("model")
    core = lax.rem(mine, 2)
    z, y, x = me // (NY * NX), lax.rem(me // NX, NY), lax.rem(me, NX)

    def there(offset):
        dz, dy, dx = offset
        return lax.rem(z + dz, NZ) * (NY * NX) + lax.rem(y + dy, NY) * NX + lax.rem(x + dx, NX)

    def span(owner):
        return pl.ds(pl.multiple_of(owner * rows, rows), rows)

    def load(m, g):
        at = pl.ds(g * group, group)
        return pltpu.make_async_copy(weights[m].at[:, at], wbuf.at[m, :, at], load_sem.at[m, g])

    for g in range(groups):
        load(0, g).start()
    small = [pltpu.make_async_copy(lows[m], low_all.at[m, :, span(me)], small_sem.at[m]) for m in range(3)]
    small.append(pltpu.make_async_copy(gain_ref, gbuf_in, small_sem.at[3]))
    highs_in = [pltpu.make_async_copy(highs[m], hbuf.at[m], small_sem.at[4 + m]) for m in range(3)]
    for copy in small + highs_in:
        copy.start()

    other_core = {"model": mine + 1 - 2 * core}
    across = {"shard": me + 1 - 2 * x, "model": lax.rem(mine + 2, 4)}
    barrier = pltpu.get_barrier_semaphore()
    for o in OFFSETS:
        pl.semaphore_signal(barrier, inc=1, device_id={"shard": there(o)}, device_id_type=MESH)
    pl.semaphore_signal(barrier, inc=1, device_id=other_core, device_id_type=MESH)
    pl.semaphore_signal(barrier, inc=1, device_id=across, device_id_type=MESH)

    def turned(m):
        for g in range(groups):
            load(m, g).wait()
            at = slice(g * group, (g + 1) * group)
            wt[m, at, :] = wbuf[m, :, at].T

    def block_copy(slot, i, o):
        m, a, n = SLOTS[slot]
        t = there(o)
        return pltpu.make_async_remote_copy(
            src_ref=wt.at[m, pl.ds(pl.multiple_of(t * cols + a * unit, 16), n * unit), :],
            dst_ref=land.at[m, pl.ds(a * unit, n * unit), span(me)],
            send_sem=send_sem.at[slot, i], recv_sem=recv_sem.at[slot, me],
            device_id={"shard": t}, device_id_type=MESH,
        )

    def sent(m):
        for slot, (of, _, _) in enumerate(SLOTS):
            if of == m:
                for i, o in enumerate(OFFSETS):
                    block_copy(slot, i, o).start()
        land[m, :, span(me)] = wt[m, pl.ds(pl.multiple_of(me * cols, 16), cols), :]

    def pair(owner, slot, target):
        return (
            pltpu.make_async_remote_copy(
                src_ref=low_all.at[:, :, span(owner)], dst_ref=low_all.at[:, :, span(owner)],
                send_sem=low_send.at[slot], recv_sem=low_recv.at[owner],
                device_id=target, device_id_type=MESH,
            ),
            pltpu.make_async_remote_copy(
                src_ref=gain_all.at[:, span(owner)], dst_ref=gain_all.at[:, span(owner)],
                send_sem=gain_send.at[slot], recv_sem=gain_recv.at[owner],
                device_id=target, device_id_type=MESH,
            ),
        )

    def launch(owner, slot, target):
        for copy in pair(owner, slot, target):
            copy.start()

    def landed(owner):
        for copy in pair(owner, 0, other_core):
            copy.wait_recv()

    def left(slot):
        for copy in pair(me, slot, other_core):
            copy.wait_send()

    flip = 1 - 2 * x

    turned(0)
    for m in (1, 2):
        for g in range(groups):
            load(m, g).start()
    for copy in small:
        copy.wait()
    gain_all[:, span(me)] = gbuf_in[...].reshape(1, rows)
    pl.semaphore_wait(barrier, N + 1)

    for i, (dz, dy) in enumerate(PLANE):
        @pl.when(core == (dz + dy) % 2)
        def _():
            launch(me, i, {"shard": there((dz, dy, 0))})
    launch(me, 15, across)
    sent(0)
    turned(1)
    sent(1)
    turned(2)
    sent(2)

    for m in range(3):
        highs_in[m].wait()
        part = hbuf[m, :, pl.ds(pl.multiple_of((me // 4) * group, group), group)]
        hrow[...] = part.astype(jnp.float32).T
        ht[m] = hrow[pl.ds(pl.multiple_of(lax.rem(me, 4) * cols, 8), cols), :].astype(ht.dtype)

    for i, (dz, dy) in enumerate(PLANE):
        @pl.when(core == (dz + dy) % 2)
        def _():
            owner = there((NZ - dz, NY - dy, 0))
            landed(owner)
            launch(owner, 16 + i, other_core)
            launch(owner, 31 + i, across)
    for i, (dz, dy) in enumerate(PLANE):
        @pl.when(core == (dz + dy) % 2)
        def _():
            owner = there((NZ - dz, NY - dy, 0)) + flip
            landed(owner)
            launch(owner, 46 + i, other_core)
    landed(me + flip)
    for i, (dz, dy) in enumerate(PLANE):
        @pl.when(core != (dz + dy) % 2)
        def _():
            landed(there((NZ - dz, NY - dy, 0)))
            landed(there((NZ - dz, NY - dy, 0)) + flip)

    def long(c):
        width = gbuf.shape[1] // CHUNKS
        return pl.ds(pl.multiple_of(c * width, width), width)

    for slot, (m, a, n) in enumerate(SLOTS):
        lines = slice(a * unit, (a + n) * unit)
        count = n * unit

        def product(c, _):
            gbuf[lines, long(c)] = jnp.dot(
                ht[m, lines, :], low_all[m, :, long(c)], preferred_element_type=jnp.float32
            )
            return 0

        lax.fori_loop(0, CHUNKS, product, 0)

        def arrive(i, _):
            source = lax.rem(me + 1 + i, N)
            pltpu.make_async_remote_copy(
                src_ref=wt.at[m, pl.ds(0, count), :],
                dst_ref=land.at[m, pl.ds(a * unit, count), span(source)],
                send_sem=send_sem.at[slot, 0], recv_sem=recv_sem.at[slot, source],
                device_id=other_core, device_id_type=MESH,
            ).wait_recv()
            return 0

        lax.fori_loop(0, N - 1, arrive, 0)

        def gained(c, top):
            at = long(c)
            r = (land[m, lines, at].astype(jnp.float32) + gbuf[lines, at]) * gain_all[:, at]
            gbuf[lines, at] = r
            r = jnp.abs(r)
            for b in range(r.shape[1] // 128):
                top = jnp.maximum(top, r[:, b * 128 : (b + 1) * 128])
            return top

        top = lax.fori_loop(0, CHUNKS, gained, jnp.zeros((count, 128), jnp.float32))
        scale = jnp.max(top, axis=1, keepdims=True)
        scale_out[m, lines, :] = jnp.broadcast_to(scale, (count, 128))
        inverse = 1.0 / scale

        def finish(c, _):
            out[m, lines, long(c)] = (gbuf[lines, long(c)] * inverse).astype(out.dtype)
            return 0

        lax.fori_loop(0, CHUNKS, finish, 0)

    for slot in range(len(SLOTS)):
        for i, o in enumerate(OFFSETS):
            block_copy(slot, i, o).wait_send()

    left(15)
    for i, (dz, dy) in enumerate(PLANE):
        @pl.when(core == (dz + dy) % 2)
        def _():
            for slot in (i, 16 + i, 31 + i, 46 + i):
                left(slot)


def deliver(out, scale, fq, fk, fv, sq, sk, sv, sem):
    half = out.shape[1] // 2
    copies = []
    for m, f in enumerate((fq, fk, fv)):
        for b in range(2):
            at = pl.ds(b * half, half)
            copy = pltpu.make_async_copy(out.at[m, at], f.at[at], sem.at[m, b])
            copy.start()
            copies.append(copy)
    for m, s in enumerate((sq, sk, sv)):
        s[...] = scale[m].T[0:1, :]
    for copy in copies:
        copy.wait()


def on_device(wq, lq, hq, wk, lk, hk, wv, lv, hv, gain):
    rows, width = wq.shape
    rank = lq.shape[1]
    cols = width // N
    total = rows * N
    slots = len(SLOTS)
    f32, bf16 = jnp.float32, jnp.bfloat16
    vmem = pl.BlockSpec(memory_space=pltpu.VMEM)
    anywhere = pl.BlockSpec(memory_space=pl.ANY)
    dma = pltpu.SemaphoreType.DMA
    out, scale = pl.pallas_call(
        exchange,
        out_shape=(
            pltpu.VMEM((3, cols, total), bf16),
            pltpu.VMEM((3, cols, 128), f32),
        ),
        in_specs=[anywhere] * 10,
        out_specs=(vmem, vmem),
        scratch_shapes=[
            pltpu.VMEM((3, rows, width), bf16),
            pltpu.VMEM((3, width, rows), bf16),
            pltpu.VMEM((3, cols, total), bf16),
            pltpu.VMEM((cols, total), f32),
            pltpu.VMEM((3, rank, total), bf16),
            pltpu.VMEM((1, total), f32),
            pltpu.VMEM((3, cols, rank), bf16),
            pltpu.VMEM((4 * cols, rank), f32),
            pltpu.VMEM((3, rank, width), bf16),
            pltpu.VMEM((rows,), f32),
            dma((3, 8)),
            dma((7,)),
            dma((slots, N)),
            dma((slots, N)),
            dma((61,)),
            dma((N,)),
            dma((61,)),
            dma((N,)),
        ],
        compiler_params=pltpu.CompilerParams(
            collective_id=0, has_side_effects=True, vmem_limit_bytes=52 * 2**20
        ),
    )(wq, wk, wv, lq.T, lk.T, lv.T, hq, hk, hv, gain)
    final = jax.ShapeDtypeStruct((cols, total), bf16)
    line = jax.ShapeDtypeStruct((1, cols), f32)
    fq, fk, fv, sq, sk, sv = pl.pallas_call(
        deliver,
        out_shape=(final, final, final, line, line, line),
        in_specs=[vmem, vmem],
        out_specs=(anywhere,) * 3 + (vmem,) * 3,
        scratch_shapes=[dma((3, 2))],
        compiler_params=pltpu.CompilerParams(vmem_limit_bytes=2 * 2**20),
    )(
        pltpu.with_memory_space_constraint(out, pltpu.VMEM),
        pltpu.with_memory_space_constraint(scale, pltpu.VMEM),
    )
    return fq.T, fk.T, fv.T, sq.reshape(cols), sk.reshape(cols), sv.reshape(cols)


def solution(mesh):
    weight, low, high = P("shard", "model"), P("shard", None), P(None, "model")
    final, scale = P(None, ("model", "shard")), P(("model", "shard"))
    return jax.shard_map(
        on_device,
        mesh=mesh,
        in_specs=(weight, low, high) * 3 + (P("shard"),),
        out_specs=(final,) * 3 + (scale,) * 3,
        check_vma=False,
    )
```

```python
import jax
import jax.numpy as jnp
from jax import lax
from jax.experimental import pallas as pl
from jax.experimental.pallas import tpu as pltpu
from jax.sharding import PartitionSpec as P

MESH = pl.DeviceIdType.MESH

NZ, NY, NX = 4, 4, 2
N = NZ * NY * NX
CUTS = (((0, 3), (3, 3)), ((0, 3), (3, 3)), ((0, 3), (3, 3)))
SLOTS = [(m, a, n) for m, cuts in enumerate(CUTS) for a, n in cuts]
CHUNKS = 8


def hops(offset):
    dz, dy, dx = offset
    return min(dz, NZ - dz) + min(dy, NY - dy) + dx


OFFSETS = sorted(
    [(dz, dy, dx) for dz in range(NZ) for dy in range(NY) for dx in range(NX)][1:],
    key=lambda o: -hops(o),
)
NEXT = [(0, 0, 1)]
REST = [o for o in OFFSETS if o not in NEXT]
PLANE = [(dz, dy) for dz in range(NZ) for dy in range(NY)][1:]


def exchange(*refs):
    weights, lows, highs, gain_ref = refs[0:3], refs[3:6], refs[6:9], refs[9]
    out, scale_out = refs[10:12]
    (wbuf, wt, land, gbuf, low_all, gain_all, ht, hrow, hbuf, gbuf_in) = refs[12:22]
    (load_sem, small_sem, send_sem, recv_sem, low_send, low_recv, gain_send, gain_recv) = refs[22:]
    rows = wbuf.shape[1]
    cols = land.shape[1]
    unit = cols // 6
    group = 4 * cols
    groups = wbuf.shape[2] // group
    me = lax.axis_index("shard")
    mine = lax.axis_index("model")
    core = lax.rem(mine, 2)
    z, y, x = me // (NY * NX), lax.rem(me // NX, NY), lax.rem(me, NX)

    def there(offset):
        dz, dy, dx = offset
        return lax.rem(z + dz, NZ) * (NY * NX) + lax.rem(y + dy, NY) * NX + lax.rem(x + dx, NX)

    def span(owner):
        return pl.ds(pl.multiple_of(owner * rows, rows), rows)

    def load(m, g):
        at = pl.ds(g * group, group)
        return pltpu.make_async_copy(weights[m].at[:, at], wbuf.at[m, :, at], load_sem.at[m, g])

    for g in range(groups):
        load(0, g).start()
    small = [pltpu.make_async_copy(lows[m], low_all.at[m, :, span(me)], small_sem.at[m]) for m in range(3)]
    small.append(pltpu.make_async_copy(gain_ref, gbuf_in, small_sem.at[3]))
    highs_in = [pltpu.make_async_copy(highs[m], hbuf.at[m], small_sem.at[4 + m]) for m in range(3)]
    for copy in small + highs_in:
        copy.start()

    other_core = {"model": mine + 1 - 2 * core}
    across = {"shard": me + 1 - 2 * x, "model": lax.rem(mine + 2, 4)}
    barrier = pltpu.get_barrier_semaphore()
    for o in OFFSETS:
        pl.semaphore_signal(barrier, inc=1, device_id={"shard": there(o)}, device_id_type=MESH)
    pl.semaphore_signal(barrier, inc=1, device_id=other_core, device_id_type=MESH)
    pl.semaphore_signal(barrier, inc=1, device_id=across, device_id_type=MESH)

    def turned(m):
        for g in range(groups):
            load(m, g).wait()
            at = slice(g * group, (g + 1) * group)
            wt[m, at, :] = wbuf[m, :, at].T

    def block_copy(slot, i, o):
        m, a, n = SLOTS[slot]
        t = there(o)
        return pltpu.make_async_remote_copy(
            src_ref=wt.at[m, pl.ds(pl.multiple_of(t * cols + a * unit, 16), n * unit), :],
            dst_ref=land.at[m, pl.ds(a * unit, n * unit), span(me)],
            send_sem=send_sem.at[slot, i], recv_sem=recv_sem.at[slot, me],
            device_id={"shard": t}, device_id_type=MESH,
        )

    def start(slots, chosen):
        for slot in slots:
            for i, o in enumerate(OFFSETS):
                if o in chosen:
                    block_copy(slot, i, o).start()

    def own(m):
        land[m, :, span(me)] = wt[m, pl.ds(pl.multiple_of(me * cols, 16), cols), :]

    def sent(m):
        start([slot for slot, (of, _, _) in enumerate(SLOTS) if of == m], REST)
        own(m)

    def pair(owner, slot, target):
        return (
            pltpu.make_async_remote_copy(
                src_ref=low_all.at[:, :, span(owner)], dst_ref=low_all.at[:, :, span(owner)],
                send_sem=low_send.at[slot], recv_sem=low_recv.at[owner],
                device_id=target, device_id_type=MESH,
            ),
            pltpu.make_async_remote_copy(
                src_ref=gain_all.at[:, span(owner)], dst_ref=gain_all.at[:, span(owner)],
                send_sem=gain_send.at[slot], recv_sem=gain_recv.at[owner],
                device_id=target, device_id_type=MESH,
            ),
        )

    def launch(owner, slot, target):
        for copy in pair(owner, slot, target):
            copy.start()

    def landed(owner):
        for copy in pair(owner, 0, other_core):
            copy.wait_recv()

    def left(slot):
        for copy in pair(me, slot, other_core):
            copy.wait_send()

    flip = 1 - 2 * x

    turned(0)
    for m in (1, 2):
        for g in range(groups):
            load(m, g).start()
    for copy in small:
        copy.wait()
    gain_all[:, span(me)] = gbuf_in[...].reshape(1, rows)
    pl.semaphore_wait(barrier, N + 1)

    start(range(2), NEXT)
    for i, (dz, dy) in enumerate(PLANE):
        @pl.when(core == (dz + dy) % 2)
        def _():
            launch(me, i, {"shard": there((dz, dy, 0))})
    launch(me, 15, across)
    sent(0)
    turned(1)
    start((2, 3), NEXT)
    sent(1)
    turned(2)
    start((4, 5), NEXT)
    sent(2)

    for m in range(3):
        highs_in[m].wait()
        part = hbuf[m, :, pl.ds(pl.multiple_of((me // 4) * group, group), group)]
        hrow[...] = part.astype(jnp.float32).T
        ht[m] = hrow[pl.ds(pl.multiple_of(lax.rem(me, 4) * cols, 8), cols), :].astype(ht.dtype)

    for i, (dz, dy) in enumerate(PLANE):
        @pl.when(core == (dz + dy) % 2)
        def _():
            owner = there((NZ - dz, NY - dy, 0))
            landed(owner)
            launch(owner, 16 + i, other_core)
            launch(owner, 31 + i, across)
    for i, (dz, dy) in enumerate(PLANE):
        @pl.when(core == (dz + dy) % 2)
        def _():
            owner = there((NZ - dz, NY - dy, 0)) + flip
            landed(owner)
            launch(owner, 46 + i, other_core)
    landed(me + flip)
    for i, (dz, dy) in enumerate(PLANE):
        @pl.when(core != (dz + dy) % 2)
        def _():
            landed(there((NZ - dz, NY - dy, 0)))
            landed(there((NZ - dz, NY - dy, 0)) + flip)

    def long(c):
        width = gbuf.shape[1] // CHUNKS
        return pl.ds(pl.multiple_of(c * width, width), width)

    for slot, (m, a, n) in enumerate(SLOTS):
        lines = slice(a * unit, (a + n) * unit)
        count = n * unit

        def product(c, _):
            gbuf[lines, long(c)] = jnp.dot(
                ht[m, lines, :], low_all[m, :, long(c)], preferred_element_type=jnp.float32
            )
            return 0

        lax.fori_loop(0, CHUNKS, product, 0)

        def waited(source):
            pltpu.make_async_remote_copy(
                src_ref=wt.at[m, pl.ds(0, count), :],
                dst_ref=land.at[m, pl.ds(a * unit, count), span(source)],
                send_sem=send_sem.at[slot, 0], recv_sem=recv_sem.at[slot, source],
                device_id=other_core, device_id_type=MESH,
            ).wait_recv()

        def arrive(i, _):
            waited(lax.rem(me + 1 + i, N))
            return 0

        def gained(at, top):
            r = (land[m, lines, at].astype(jnp.float32) + gbuf[lines, at]) * gain_all[:, at]
            gbuf[lines, at] = r
            r = jnp.abs(r)
            for b in range(r.shape[1] // 128):
                top = jnp.maximum(top, r[:, b * 128 : (b + 1) * 128])
            return top

        top = jnp.zeros((count, 128), jnp.float32)
        if slot < len(SLOTS) - 1:
            lax.fori_loop(0, N - 1, arrive, 0)
            top = lax.fori_loop(0, CHUNKS, lambda c, top: gained(long(c), top), top)
        else:
            top = gained(span(me), top)
            for dz, dy, dx in NEXT + REST:
                source = there((NZ - dz, NY - dy, NX - dx))
                waited(source)
                top = gained(span(source), top)
        scale = jnp.max(top, axis=1, keepdims=True)
        scale_out[m, lines, :] = jnp.broadcast_to(scale, (count, 128))
        inverse = 1.0 / scale

        def finish(c, _):
            out[m, lines, long(c)] = (gbuf[lines, long(c)] * inverse).astype(out.dtype)
            return 0

        lax.fori_loop(0, CHUNKS, finish, 0)

    for slot in range(len(SLOTS)):
        for i, o in enumerate(OFFSETS):
            block_copy(slot, i, o).wait_send()

    left(15)
    for i, (dz, dy) in enumerate(PLANE):
        @pl.when(core == (dz + dy) % 2)
        def _():
            for slot in (i, 16 + i, 31 + i, 46 + i):
                left(slot)


def deliver(out, scale, fq, fk, fv, sq, sk, sv, line, sem, line_sem):
    half = out.shape[1] // 2
    copies = []
    for m, f in enumerate((fq, fk, fv)):
        for b in range(2):
            at = pl.ds(b * half, half)
            copies.append(pltpu.make_async_copy(out.at[m, at], f.at[at], sem.at[m, b]))
            copies[-1].start()
    for m, s in enumerate((sq, sk, sv)):
        line[m] = scale[m].T[0:1, :]
        copies.append(pltpu.make_async_copy(line.at[m], s, line_sem.at[m]))
    for copy in copies[6:]:
        copy.start()
    for copy in copies:
        copy.wait()


def on_device(wq, lq, hq, wk, lk, hk, wv, lv, hv, gain):
    rows, width = wq.shape
    rank = lq.shape[1]
    cols = width // N
    total = rows * N
    slots = len(SLOTS)
    f32, bf16 = jnp.float32, jnp.bfloat16
    vmem = pl.BlockSpec(memory_space=pltpu.VMEM)
    anywhere = pl.BlockSpec(memory_space=pl.ANY)
    dma = pltpu.SemaphoreType.DMA
    out, scale = pl.pallas_call(
        exchange,
        out_shape=(
            pltpu.VMEM((3, cols, total), bf16),
            pltpu.VMEM((3, cols, 128), f32),
        ),
        in_specs=[anywhere] * 10,
        out_specs=(vmem, vmem),
        scratch_shapes=[
            pltpu.VMEM((3, rows, width), bf16),
            pltpu.VMEM((3, width, rows), bf16),
            pltpu.VMEM((3, cols, total), bf16),
            pltpu.VMEM((cols, total), f32),
            pltpu.VMEM((3, rank, total), bf16),
            pltpu.VMEM((1, total), f32),
            pltpu.VMEM((3, cols, rank), bf16),
            pltpu.VMEM((4 * cols, rank), f32),
            pltpu.VMEM((3, rank, width), bf16),
            pltpu.VMEM((rows,), f32),
            dma((3, 8)),
            dma((7,)),
            dma((slots, N)),
            dma((slots, N)),
            dma((61,)),
            dma((N,)),
            dma((61,)),
            dma((N,)),
        ],
        compiler_params=pltpu.CompilerParams(
            collective_id=0, has_side_effects=True, vmem_limit_bytes=52 * 2**20
        ),
    )(wq, wk, wv, lq.T, lk.T, lv.T, hq, hk, hv, gain)
    final = jax.ShapeDtypeStruct((cols, total), bf16)
    line = jax.ShapeDtypeStruct((1, cols), f32)
    fq, fk, fv, sq, sk, sv = pl.pallas_call(
        deliver,
        out_shape=(final, final, final, line, line, line),
        in_specs=[vmem, vmem],
        out_specs=(anywhere,) * 6,
        scratch_shapes=[pltpu.VMEM((3, 1, cols), f32), dma((3, 2)), dma((3,))],
        compiler_params=pltpu.CompilerParams(vmem_limit_bytes=2 * 2**20),
    )(
        pltpu.with_memory_space_constraint(out, pltpu.VMEM),
        pltpu.with_memory_space_constraint(scale, pltpu.VMEM),
    )
    return fq.T, fk.T, fv.T, sq.reshape(cols), sk.reshape(cols), sv.reshape(cols)


def solution(mesh):
    weight, low, high = P("shard", "model"), P("shard", None), P(None, "model")
    final, scale = P(None, ("model", "shard")), P(("model", "shard"))
    return jax.shard_map(
        on_device,
        mesh=mesh,
        in_specs=(weight, low, high) * 3 + (P("shard"),),
        out_specs=(final,) * 3 + (scale,) * 3,
        check_vma=False,
    )
```

```python
import jax
import jax.numpy as jnp
from jax import lax
from jax.experimental import pallas as pl
from jax.experimental.pallas import tpu as pltpu
from jax.sharding import PartitionSpec as P

MESH = pl.DeviceIdType.MESH

NZ, NY, NX = 4, 4, 2
N = NZ * NY * NX
CUTS = (((0, 3), (3, 3)), ((0, 3), (3, 3)), ((0, 3), (3, 3)))
SLOTS = [(m, a, n) for m, cuts in enumerate(CUTS) for a, n in cuts]
CHUNKS = 8


def hops(offset):
    dz, dy, dx = offset
    return min(dz, NZ - dz) + min(dy, NY - dy) + dx


OFFSETS = sorted(
    [(dz, dy, dx) for dz in range(NZ) for dy in range(NY) for dx in range(NX)][1:],
    key=lambda o: -hops(o),
)
NEXT = [(0, 0, 1)]
REST = [o for o in OFFSETS if o not in NEXT]
PLANE = [(dz, dy) for dz in range(NZ) for dy in range(NY)][1:]


def exchange(*refs):
    weights, lows, highs, gain_ref = refs[0:3], refs[3:6], refs[6:9], refs[9]
    out, scale_out = refs[10:12]
    (wbuf, wt, land, gbuf, low_all, gain_all, ht, hrow, hbuf, gbuf_in) = refs[12:22]
    (load_sem, small_sem, send_sem, recv_sem, low_send, low_recv, gain_send, gain_recv) = refs[22:]
    rows = wbuf.shape[1]
    cols = land.shape[1]
    unit = cols // 6
    group = 4 * cols
    groups = wbuf.shape[2] // group
    me = lax.axis_index("shard")
    mine = lax.axis_index("model")
    core = lax.rem(mine, 2)
    z, y, x = me // (NY * NX), lax.rem(me // NX, NY), lax.rem(me, NX)

    def there(offset):
        dz, dy, dx = offset
        return lax.rem(z + dz, NZ) * (NY * NX) + lax.rem(y + dy, NY) * NX + lax.rem(x + dx, NX)

    def span(owner):
        return pl.ds(pl.multiple_of(owner * rows, rows), rows)

    def load(m, g):
        at = pl.ds(g * group, group)
        return pltpu.make_async_copy(weights[m].at[:, at], wbuf.at[m, :, at], load_sem.at[m, g])

    for g in range(groups):
        load(0, g).start()
    small = [pltpu.make_async_copy(lows[m], low_all.at[m, :, span(me)], small_sem.at[m]) for m in range(3)]
    small.append(pltpu.make_async_copy(gain_ref, gbuf_in, small_sem.at[3]))
    highs_in = [pltpu.make_async_copy(highs[m], hbuf.at[m], small_sem.at[4 + m]) for m in range(3)]
    for copy in small + highs_in:
        copy.start()

    other_core = {"model": mine + 1 - 2 * core}
    across = {"shard": me + 1 - 2 * x, "model": lax.rem(mine + 2, 4)}
    barrier = pltpu.get_barrier_semaphore()
    for o in OFFSETS:
        pl.semaphore_signal(barrier, inc=1, device_id={"shard": there(o)}, device_id_type=MESH)
    pl.semaphore_signal(barrier, inc=1, device_id=other_core, device_id_type=MESH)
    pl.semaphore_signal(barrier, inc=1, device_id=across, device_id_type=MESH)

    def turned(m):
        for g in range(groups):
            load(m, g).wait()
            at = slice(g * group, (g + 1) * group)
            wt[m, at, :] = wbuf[m, :, at].T

    def block_copy(slot, i, o):
        m, a, n = SLOTS[slot]
        t = there(o)
        return pltpu.make_async_remote_copy(
            src_ref=wt.at[m, pl.ds(pl.multiple_of(t * cols + a * unit, 16), n * unit), :],
            dst_ref=land.at[m, pl.ds(a * unit, n * unit), span(me)],
            send_sem=send_sem.at[slot, i], recv_sem=recv_sem.at[slot, me],
            device_id={"shard": t}, device_id_type=MESH,
        )

    def start(slots, chosen):
        for slot in slots:
            for i, o in enumerate(OFFSETS):
                if o in chosen:
                    block_copy(slot, i, o).start()

    def own(m):
        land[m, :, span(me)] = wt[m, pl.ds(pl.multiple_of(me * cols, 16), cols), :]

    def sent(m):
        start([slot for slot, (of, _, _) in enumerate(SLOTS) if of == m], REST)
        own(m)

    def pair(owner, slot, target):
        return (
            pltpu.make_async_remote_copy(
                src_ref=low_all.at[:, :, span(owner)], dst_ref=low_all.at[:, :, span(owner)],
                send_sem=low_send.at[slot], recv_sem=low_recv.at[owner],
                device_id=target, device_id_type=MESH,
            ),
            pltpu.make_async_remote_copy(
                src_ref=gain_all.at[:, span(owner)], dst_ref=gain_all.at[:, span(owner)],
                send_sem=gain_send.at[slot], recv_sem=gain_recv.at[owner],
                device_id=target, device_id_type=MESH,
            ),
        )

    def launch(owner, slot, target):
        for copy in pair(owner, slot, target):
            copy.start()

    def landed(owner):
        for copy in pair(owner, 0, other_core):
            copy.wait_recv()

    def left(slot):
        for copy in pair(me, slot, other_core):
            copy.wait_send()

    flip = 1 - 2 * x

    turned(0)
    for m in (1, 2):
        for g in range(groups):
            load(m, g).start()
    for copy in small:
        copy.wait()
    gain_all[:, span(me)] = gbuf_in[...].reshape(1, rows)
    pl.semaphore_wait(barrier, N + 1)

    start(range(2), NEXT)
    for i, (dz, dy) in enumerate(PLANE):
        @pl.when(core == (dz + dy) % 2)
        def _():
            launch(me, i, {"shard": there((dz, dy, 0))})
    launch(me, 15, across)
    sent(0)
    turned(1)
    start((2, 3), NEXT)
    sent(1)
    turned(2)
    start((4, 5), NEXT)
    sent(2)

    for m in range(3):
        highs_in[m].wait()
        part = hbuf[m, :, pl.ds(pl.multiple_of((me // 4) * group, group), group)]
        hrow[...] = part.astype(jnp.float32).T
        ht[m] = hrow[pl.ds(pl.multiple_of(lax.rem(me, 4) * cols, 8), cols), :].astype(ht.dtype)

    for i, (dz, dy) in enumerate(PLANE):
        @pl.when(core == (dz + dy) % 2)
        def _():
            owner = there((NZ - dz, NY - dy, 0))
            landed(owner)
            launch(owner, 16 + i, other_core)
            launch(owner, 31 + i, across)
    for i, (dz, dy) in enumerate(PLANE):
        @pl.when(core == (dz + dy) % 2)
        def _():
            owner = there((NZ - dz, NY - dy, 0)) + flip
            landed(owner)
            launch(owner, 46 + i, other_core)
    landed(me + flip)
    for i, (dz, dy) in enumerate(PLANE):
        @pl.when(core != (dz + dy) % 2)
        def _():
            landed(there((NZ - dz, NY - dy, 0)))
            landed(there((NZ - dz, NY - dy, 0)) + flip)

    def long(c):
        width = gbuf.shape[1] // CHUNKS
        return pl.ds(pl.multiple_of(c * width, width), width)

    def settled():
        for slot in range(len(SLOTS) - 1):
            for i, o in enumerate(OFFSETS):
                block_copy(slot, i, o).wait_send()
        left(15)
        for i, (dz, dy) in enumerate(PLANE):
            @pl.when(core == (dz + dy) % 2)
            def _():
                for slot in (i, 16 + i, 31 + i, 46 + i):
                    left(slot)

    for slot, (m, a, n) in enumerate(SLOTS):
        lines = slice(a * unit, (a + n) * unit)
        count = n * unit

        def product(c, _):
            gbuf[lines, long(c)] = jnp.dot(
                ht[m, lines, :], low_all[m, :, long(c)], preferred_element_type=jnp.float32
            )
            return 0

        lax.fori_loop(0, CHUNKS, product, 0)

        if slot == len(SLOTS) - 1:
            settled()

        def waited(source):
            pltpu.make_async_remote_copy(
                src_ref=wt.at[m, pl.ds(0, count), :],
                dst_ref=land.at[m, pl.ds(a * unit, count), span(source)],
                send_sem=send_sem.at[slot, 0], recv_sem=recv_sem.at[slot, source],
                device_id=other_core, device_id_type=MESH,
            ).wait_recv()

        def arrive(i, _):
            waited(lax.rem(me + 1 + i, N))
            return 0

        def gained(at, top):
            r = (land[m, lines, at].astype(jnp.float32) + gbuf[lines, at]) * gain_all[:, at]
            gbuf[lines, at] = r
            r = jnp.abs(r)
            for b in range(r.shape[1] // 128):
                top = jnp.maximum(top, r[:, b * 128 : (b + 1) * 128])
            return top

        top = jnp.zeros((count, 128), jnp.float32)
        if slot < len(SLOTS) - 1:
            lax.fori_loop(0, N - 1, arrive, 0)
            top = lax.fori_loop(0, CHUNKS, lambda c, top: gained(long(c), top), top)
        else:
            top = gained(span(me), top)
            for dz, dy, dx in NEXT + REST:
                source = there((NZ - dz, NY - dy, NX - dx))
                waited(source)
                top = gained(span(source), top)
        scale = jnp.max(top, axis=1, keepdims=True)
        scale_out[m, lines, :] = jnp.broadcast_to(scale, (count, 128))
        inverse = 1.0 / scale

        def finish(c, _):
            out[m, lines, long(c)] = (gbuf[lines, long(c)] * inverse).astype(out.dtype)
            return 0

        lax.fori_loop(0, CHUNKS, finish, 0)

    for i, o in enumerate(OFFSETS):
        block_copy(len(SLOTS) - 1, i, o).wait_send()


def deliver(out, scale, fq, fk, fv, sq, sk, sv, line, sem, line_sem):
    half = out.shape[1] // 2
    copies = []
    for m, f in enumerate((fq, fk, fv)):
        for b in range(2):
            at = pl.ds(b * half, half)
            copies.append(pltpu.make_async_copy(out.at[m, at], f.at[at], sem.at[m, b]))
            copies[-1].start()
    for m, s in enumerate((sq, sk, sv)):
        line[m] = scale[m].T[0:1, :]
        copies.append(pltpu.make_async_copy(line.at[m], s, line_sem.at[m]))
    for copy in copies[6:]:
        copy.start()
    for copy in copies:
        copy.wait()


def on_device(wq, lq, hq, wk, lk, hk, wv, lv, hv, gain):
    rows, width = wq.shape
    rank = lq.shape[1]
    cols = width // N
    total = rows * N
    slots = len(SLOTS)
    f32, bf16 = jnp.float32, jnp.bfloat16
    vmem = pl.BlockSpec(memory_space=pltpu.VMEM)
    anywhere = pl.BlockSpec(memory_space=pl.ANY)
    dma = pltpu.SemaphoreType.DMA
    out, scale = pl.pallas_call(
        exchange,
        out_shape=(
            pltpu.VMEM((3, cols, total), bf16),
            pltpu.VMEM((3, cols, 128), f32),
        ),
        in_specs=[anywhere] * 10,
        out_specs=(vmem, vmem),
        scratch_shapes=[
            pltpu.VMEM((3, rows, width), bf16),
            pltpu.VMEM((3, width, rows), bf16),
            pltpu.VMEM((3, cols, total), bf16),
            pltpu.VMEM((cols, total), f32),
            pltpu.VMEM((3, rank, total), bf16),
            pltpu.VMEM((1, total), f32),
            pltpu.VMEM((3, cols, rank), bf16),
            pltpu.VMEM((4 * cols, rank), f32),
            pltpu.VMEM((3, rank, width), bf16),
            pltpu.VMEM((rows,), f32),
            dma((3, 8)),
            dma((7,)),
            dma((slots, N)),
            dma((slots, N)),
            dma((61,)),
            dma((N,)),
            dma((61,)),
            dma((N,)),
        ],
        compiler_params=pltpu.CompilerParams(
            collective_id=0, has_side_effects=True, vmem_limit_bytes=52 * 2**20
        ),
    )(wq, wk, wv, lq.T, lk.T, lv.T, hq, hk, hv, gain)
    final = jax.ShapeDtypeStruct((cols, total), bf16)
    line = jax.ShapeDtypeStruct((1, cols), f32)
    fq, fk, fv, sq, sk, sv = pl.pallas_call(
        deliver,
        out_shape=(final, final, final, line, line, line),
        in_specs=[vmem, vmem],
        out_specs=(anywhere,) * 6,
        scratch_shapes=[pltpu.VMEM((3, 1, cols), f32), dma((3, 2)), dma((3,))],
        compiler_params=pltpu.CompilerParams(vmem_limit_bytes=2 * 2**20),
    )(
        pltpu.with_memory_space_constraint(out, pltpu.VMEM),
        pltpu.with_memory_space_constraint(scale, pltpu.VMEM),
    )
    return fq.T, fk.T, fv.T, sq.reshape(cols), sk.reshape(cols), sv.reshape(cols)


def solution(mesh):
    weight, low, high = P("shard", "model"), P("shard", None), P(None, "model")
    final, scale = P(None, ("model", "shard")), P(("model", "shard"))
    return jax.shard_map(
        on_device,
        mesh=mesh,
        in_specs=(weight, low, high) * 3 + (P("shard"),),
        out_specs=(final,) * 3 + (scale,) * 3,
        check_vma=False,
    )
```
